32 devices in a mesh: rep: 1, r: 8 (over y, z), s: 4 (over x, core).
Axes of the slice: x: 2, y: 2, z: 4, core: 2. Of those that a mesh axis runs over, the one named last changes fastest.
Arguments:
- x: bfloat16 [32, 4096, 768], P(('rep', 'r', 's'))
- dy: bfloat16 [32, 4096, 768], P(('rep', 'r', 's'))
- w_gate: bfloat16 [2, 768, 1792], P(None, 's')
- w_up: bfloat16 [2, 768, 1792], P(None, 's')
- w_down: bfloat16 [2, 1792, 768], P(None, 's')
Outputs:
- output 1: bfloat16 [32, 4096, 768], P(('rep', 'r', 's'))
- output 2: bfloat16 [2, 768, 1792], P('rep', 's')
- output 3: bfloat16 [2, 768, 1792], P('rep', 's')
- output 4: bfloat16 [2, 1792, 768], P('rep', 's')
All inputs are finite; a program needn't handle non-finite values.
Results may differ from the reference program's by a relative error of at most 0.018.
Values are sent between devices in bfloat16 or wider.
A program may use at most 2 GiB of HBM per device.

```python
import jax
import jax.numpy as jnp
from jax import lax

SEQUENCES = 32
TOKENS = 4096
D = 768
FF = 1792
LAYERS = 2
NAMES = ("w_gate", "w_up", "w_down")
SHAPES = {"w_gate": (LAYERS, D, FF), "w_up": (LAYERS, D, FF), "w_down": (LAYERS, FF, D)}


def bump(key, n, height):
    away = (jnp.arange(n, dtype=jnp.int32) - jax.random.randint(key, (), 0, n, jnp.int32)) % n
    return jnp.where(away < n // 8, height, 1.0)


def together(key, own, strength):
    shared = jax.random.normal(key, own.shape[1:], jnp.float32)
    return (own + strength * shared) * lax.rsqrt(1 + strength * strength)


def setup_inputs(seed: int = 0, part: int = 0) -> dict:
    kx, kdy, ka, kb, kz, kf, kh, kl, *kw = jax.random.split(jax.random.key(seed), 8 + len(NAMES))
    kx, kdy, ka, kb = (jax.random.fold_in(k, part) for k in (kx, kdy, ka, kb))
    shape = (SEQUENCES, TOKENS, D)
    much_x, much_dy = jax.random.uniform(kz, (2,), jnp.float32, 0.0, 1.0)
    layers = 2.0 ** jax.random.uniform(kl, (LAYERS, 1, 1), jnp.float32, -1.0, 1.0)
    x = together(ka, jax.random.normal(kx, shape, jnp.float32), much_x) * bump(kf, D, 4.0)
    dy = together(kb, jax.random.normal(kdy, shape, jnp.float32), much_dy)
    drawn = {"x": x.astype(jnp.bfloat16), "dy": (dy * (SEQUENCES * TOKENS) ** -0.5).astype(jnp.bfloat16)}
    for key, name in zip(kw, NAMES, strict=True):
        w = jax.random.normal(key, SHAPES[name], jnp.float32) * SHAPES[name][1] ** -0.5
        drawn[name] = (w * {"w_gate": 1.0, "w_up": bump(kh, FF, 4.0), "w_down": layers}[name]).astype(jnp.bfloat16)
    return drawn


def matmul(a, w):
    return jnp.dot(a, w, preferred_element_type=jnp.float32).astype(jnp.bfloat16)


def normed(h):
    wide = h.astype(jnp.float32)
    scale = lax.rsqrt(jnp.mean(wide**2, -1, keepdims=True) + 1e-6)
    return (wide * scale).astype(jnp.bfloat16)


def layer(h, w):
    a = normed(h)
    gate = jnp.dot(a, w["w_gate"], preferred_element_type=jnp.float32)
    up = jnp.dot(a, w["w_up"], preferred_element_type=jnp.float32)
    return h + matmul((jax.nn.silu(gate) * up).astype(jnp.bfloat16), w["w_down"])


def stack(weights, h):
    return lax.scan(lambda h, w: (layer(h, w), None), h, weights)[0]


def reference(x, dy, w_gate, w_up, w_down):
    weights = dict(zip(NAMES, (w_gate, w_up, w_down), strict=True))

    def take(so_far, sequence):
        h, by_y = sequence
        _, back = jax.vjp(stack, weights, h)
        by_weights, by_h = back(by_y)
        return jax.tree.map(lambda total, term: total + term.astype(jnp.float32), so_far, by_weights), by_h

    none_yet = {name: jnp.zeros(w.shape, jnp.float32) for name, w in weights.items()}
    by_weights, by_x = lax.scan(take, none_yet, (x, dy))
    return (by_x, *(by_weights[name].astype(jnp.bfloat16) for name in NAMES))
```

```python
import functools
import jax
import jax.numpy as jnp
from jax import lax
from jax.experimental import pallas as pl
from jax.experimental.pallas import tpu as pltpu
from jax.sharding import PartitionSpec as P

F32, BF = jnp.float32, jnp.bfloat16
MESH = pl.DeviceIdType.MESH
TOK, D, FF = 4096, 768, 1792
T = TOK // 8
ANY = pl.BlockSpec(memory_space=pl.ANY)


def dot(a, b):
    return jnp.dot(a, b, preferred_element_type=F32)


def dot_nt(a, b):
    return lax.dot_general(a, b, (((1,), (1,)), ((), ())), preferred_element_type=F32)


def dot_tn(a, b):
    return lax.dot_general(a, b, (((0,), (0,)), ((), ())), preferred_element_type=F32)


def sigmoid(g):
    return 0.5 + 0.5 * jnp.tanh(0.5 * g)


def place():
    r, s = lax.axis_index("r"), lax.axis_index("s")
    return r, r // 4, lax.rem(r, 4), s, s // 2, lax.rem(s, 2)


def forward_kernel(x_hbm, wg_in, wu_in, wd_in,
                   h1_hbm, gate_hbm, up_hbm, at_hbm, w0g, w0u, w0d, w1g, w1u, w1d,
                   wg_v, wu_v, wd_v, og, ou, od, a_v, gate_v, hin, up_s, at_s, hid_s, h1_s,
                   sa_s, sa_r, sr_s, sr_r, sp_s, sp_r, so_s, so_r, s_loc, s_hin, s_up, s_at, s_h1, s_gate, s_w0):
    r, y, z, s, x, c = place()
    colour = lax.rem(y + z, 2)
    partner = {"s": 2 * x + (1 - c)}
    across = {"s": 2 * (1 - x) + c}
    beside = ({"r": lax.rem(r + 4, 8)}, {"r": r + 1 - 2 * lax.rem(z, 2)})
    mine, theirs, others = 2 * x + c, 2 * (1 - x) + c, 2 * (1 - x) + (1 - c)
    shards = (wg_in, wu_in, wd_in)
    whole = (wg_v, wu_v, wd_v, w1g, w1u, w1d)
    rows = (192, 192, 448, 192, 192, 448)

    def piece(m, q, half, k):
        n = rows[m] // 4
        return whole[m].at[pl.ds(pl.multiple_of(q * rows[m] + half * (2 * n) + k * n, 16), n)]

    def quarter(m, q):
        return whole[m].at[pl.ds(pl.multiple_of(q * rows[m], 16), rows[m])]

    def remote(src, dst, send, recv, to):
        return pltpu.make_async_remote_copy(src_ref=src, dst_ref=dst, send_sem=send, recv_sem=recv, device_id=to, device_id_type=MESH)

    def first(m, k):
        n = rows[m] // 4
        src = shards[m % 3].at[m // 3, pl.ds(pl.multiple_of(colour * (2 * n) + k * n, 16), n)]
        return remote(src, piece(m, mine, colour, k), sa_s.at[m, k], sa_r.at[m, k], across)

    def own(m):
        return remote(shards[m % 3].at[m // 3], quarter(m, mine), so_s.at[m], so_r.at[m], partner)

    def relay(m, k):
        p = piece(m, theirs, colour, k)
        return remote(p, p, sr_s.at[m, k], sr_r.at[m, k], beside[k])

    def pass_on(m, j, k):
        p = piece(m, theirs, colour if j == 0 else 1 - colour, k)
        return remote(p, p, sp_s.at[m, j, k], sp_r.at[m, j, k], partner)

    def arrived(copy):
        copy.wait_recv()

    def at_first(m, k):
        remote(piece(m, theirs, colour, k), piece(m, theirs, colour, k), sa_s.at[m, k], sa_r.at[m, k], across).wait_recv()
        relay(m, k).start()
        pass_on(m, 0, k).start()

    def at_beside(m, k):
        p = piece(m, theirs, 1 - colour, k)
        remote(p, p, sr_s.at[m, k], sr_r.at[m, k], beside[k]).wait_recv()
        pass_on(m, 1, k).start()

    def at_end(m):
        q = quarter(m, 2 * x + (1 - c))
        remote(q, q, so_s.at[m], so_r.at[m], partner).wait_recv()
        for j in range(2):
            for k in range(2):
                p = piece(m, others, colour if j == 0 else 1 - colour, k)
                remote(p, p, sp_s.at[m, j, k], sp_r.at[m, j, k], partner).wait_recv()

    barrier = pltpu.get_barrier_semaphore()
    for to in (partner, across, *beside):
        pl.semaphore_signal(barrier, inc=1, device_id=to, device_id_type=MESH)

    loads = []
    for m in range(3):
        loads.append(pltpu.make_async_copy(shards[m].at[0], quarter(m, mine), s_loc.at[m]))
        loads.append(pltpu.make_async_copy(shards[m].at[1], (og, ou, od)[m], s_loc.at[3 + m]))
    for copy in loads:
        copy.start()

    def load_h(i):
        return pltpu.make_async_copy(x_hbm.at[pl.ds(i * T, T)], hin.at[lax.rem(i, 2)], s_hin.at[lax.rem(i, 2)])

    load_h(0).start()
    pl.semaphore_wait(barrier, 4)
    for m in range(6):
        for k in range(2):
            first(m, k).start()
        own(m).start()

    def store_at(i):
        return pltpu.make_async_copy(at_s.at[lax.rem(i, 2)], at_hbm.at[:, pl.ds(pl.multiple_of(i * T, T), T)], s_at.at[lax.rem(i, 2)])

    @pl.loop(0, 8)
    def _(i):
        load_h(i).wait()

        @pl.when(i < 7)
        def _():
            load_h(i + 1).start()

        @pl.when(i >= 2)
        def _():
            store_at(i - 2).wait()

        h = hin[lax.rem(i, 2)].astype(F32)
        a = (h * lax.rsqrt(jnp.mean(h * h, -1, keepdims=True) + 1e-6)).astype(BF)
        a_v[pl.ds(i * T, T)] = a
        at_s[lax.rem(i, 2)] = a.T
        store_at(i).start()

    store_at(6).wait()
    store_at(7).wait()
    for copy in loads:
        copy.wait()
    saves = [pltpu.make_async_copy((og, ou, od)[m], quarter(3 + m, mine), s_loc.at[m]) for m in range(3)]
    for copy in saves:
        copy.start()

    for k in range(2):
        at_first(0, k)
    for k in range(2):
        at_beside(0, k)
    at_end(0)

    w0_out = [pltpu.make_async_copy(whole[m], (w0g, w0u, w0d)[m], s_w0.at[m]) for m in range(3)]
    w0_out[0].start()

    def store_gate(i):
        return pltpu.make_async_copy(gate_v.at[pl.ds(i * T, T)], gate_hbm.at[pl.ds(i * T, T)], s_gate.at[i])

    ACTS1 = {0: [(at_first, 1, 0)], 2: [(at_first, 1, 1)], 4: [(at_beside, 1, 0), (at_first, 2, 0)], 6: [(at_beside, 1, 1), (at_first, 2, 1)]}
    ACTS2 = {0: [(at_beside, 2, 0), (at_beside, 2, 1), (at_first, 3, 0), (at_first, 3, 1)], 2: [(at_beside, 3, 0), (at_first, 4, 0)],
             3: [(at_beside, 3, 1), (at_first, 4, 1)], 4: [(at_beside, 4, 0), (at_first, 5, 0)], 5: [(at_beside, 4, 1), (at_first, 5, 1)],
             6: [(at_beside, 5, 0)], 7: [(at_beside, 5, 1)]}

    def act(acts, i):
        for step, todo in acts.items():
            @pl.when(i == step)
            def _():
                for f, m, k in todo:
                    f(m, k)

    @pl.loop(0, 8)
    def _(i):
        act(ACTS1, i)
        for half in range(2):
            rs = pl.ds(pl.multiple_of(i * T + half * (T // 2), T // 2), T // 2)
            a = a_v[rs]
            for n in range(7):
                gate_v[rs, n * 256:(n + 1) * 256] = dot(a, wg_v[:, n * 256:(n + 1) * 256])
        store_gate(i).start()

    at_end(1)
    w0_out[1].start()

    def store_up(i):
        return pltpu.make_async_copy(up_s.at[lax.rem(i, 2)], up_hbm.at[pl.ds(i * T, T)], s_up.at[lax.rem(i, 2)])

    def store_h1(i):
        return pltpu.make_async_copy(h1_s.at[lax.rem(i, 2)], h1_hbm.at[pl.ds(i * T, T)], s_h1.at[lax.rem(i, 2)])

    load_h(0).start()

    @pl.loop(0, 8)
    def _(i):
        act(ACTS2, i)
        load_h(i).wait()

        @pl.when(i < 7)
        def _():
            load_h(i + 1).start()

        @pl.when(i >= 2)
        def _():
            store_up(i - 2).wait()
            store_h1(i - 2).wait()

        @pl.when(i == 0)
        def _():
            at_end(2)
            w0_out[2].start()

        slot = lax.rem(i, 2)
        for half in range(2):
            lo = half * (T // 2)
            rs = pl.ds(pl.multiple_of(i * T + lo, T // 2), T // 2)
            a = a_v[rs]
            for n in range(7):
                cs = slice(n * 256, (n + 1) * 256)
                g = gate_v[rs, cs]
                u = dot(a, wu_v[:, cs])
                up_s[slot, lo:lo + T // 2, cs] = u
                hid_s[lo:lo + T // 2, cs] = (g * sigmoid(g) * u).astype(BF)
        for half in range(2):
            lo = half * (T // 2)
            o = dot(hid_s[lo:lo + T // 2], wd_v[...]).astype(BF)
            h1_s[slot, lo:lo + T // 2] = hin[slot, lo:lo + T // 2] + o
        store_up(i).start()
        store_h1(i).start()

    for m in range(3, 6):
        at_end(m)
    for i in (6, 7):
        store_up(i).wait()
        store_h1(i).wait()
    for i in range(8):
        store_gate(i).wait()
    for copy in w0_out + saves:
        copy.wait()
    for m in range(6):
        own(m).wait_send()
        for k in range(2):
            first(m, k).wait_send()
            relay(m, k).wait_send()
            for j in range(2):
                pass_on(m, j, k).wait_send()


def forward(x, wg, wu, wd):
    S = jax.ShapeDtypeStruct
    dma = pltpu.SemaphoreType.DMA
    return pl.pallas_call(
        forward_kernel,
        out_shape=(S((TOK, D), BF), S((TOK, FF), F32), S((TOK, FF), F32), S((D, TOK), BF),
                   S((D, FF), BF), S((D, FF), BF), S((FF, D), BF), S((D, FF), BF), S((D, FF), BF), S((FF, D), BF)),
        in_specs=[ANY] * 4,
        out_specs=(ANY,) * 10,
        scratch_shapes=[
            pltpu.VMEM((D, FF), BF), pltpu.VMEM((D, FF), BF), pltpu.VMEM((FF, D), BF),
            pltpu.VMEM((192, FF), BF), pltpu.VMEM((192, FF), BF), pltpu.VMEM((448, D), BF),
            pltpu.VMEM((TOK, D), BF), pltpu.VMEM((TOK, FF), F32),
            pltpu.VMEM((2, T, D), BF), pltpu.VMEM((2, T, FF), F32), pltpu.VMEM((2, D, T), BF),
            pltpu.VMEM((T, FF), BF), pltpu.VMEM((2, T, D), BF),
            dma((6, 2)), dma((6, 2)), dma((6, 2)), dma((6, 2)), dma((6, 2, 2)), dma((6, 2, 2)), dma((6,)), dma((6,)),
            dma((6,)), dma((2,)), dma((2,)), dma((2,)), dma((2,)), dma((8,)), dma((3,)),
        ],
        compiler_params=pltpu.CompilerParams(collective_id=0, has_side_effects=True, vmem_limit_bytes=67_000_000),
        cost_estimate=pl.CostEstimate(flops=6 * TOK * D * FF, bytes_accessed=120_000_000, transcendentals=TOK * FF),
        name="forward",
    )(x, wg, wu, wd)


def full(shape):
    return pl.BlockSpec(shape, lambda i: (0,) * len(shape), pipeline_mode=pl.Buffered(1))


def tile(t, n):
    return pl.BlockSpec((t, n), lambda i: (i, 0))


def norm_back(da, h, dy):
    h, da = h.astype(F32), da.astype(BF).astype(F32)
    scale = lax.rsqrt(jnp.mean(h * h, -1, keepdims=True) + 1e-6)
    along = jnp.sum(da * h, -1, keepdims=True) * (scale * scale * scale * (1.0 / D))
    return dy + (da * scale - h * along).astype(BF)


def last_kernel(h_ref, dy_ref, wg, wu, wd, dh_ref, dg_ref, du_ref, dwd, at_ref, a_s, hid_s):
    n_rows = h_ref.shape[0]
    for lo in range(0, n_rows, 512):
        r = slice(lo, lo + 512)
        h = h_ref[r].astype(F32)
        a_s[r] = (h * lax.rsqrt(jnp.mean(h * h, -1, keepdims=True) + 1e-6)).astype(BF)
    for lo in range(0, n_rows, 512):
        r = slice(lo, lo + 512)
        for n in range(7):
            cs = slice(n * 256, (n + 1) * 256)
            g, u = dot(a_s[r], wg[:, cs]), dot(a_s[r], wu[:, cs])
            back = dot_nt(dy_ref[r], wd[cs]).astype(BF).astype(F32)
            s = sigmoid(g)
            silu = g * s
            hid_s[r, cs] = (silu * u).astype(BF)
            dg_ref[r, cs] = (back * u * (s + silu * (1 - s))).astype(BF)
            du_ref[r, cs] = (back * silu).astype(BF)
    for lo in range(0, n_rows, 256):
        r = slice(lo, lo + 256)
        dh_ref[r] = norm_back(dot_nt(dg_ref[r], wg[...]) + dot_nt(du_ref[r], wu[...]), h_ref[r], dy_ref[r])
    at_ref[...] = a_s[...].T

    @pl.when(pl.program_id(0) == 0)
    def _():
        dwd[...] = jnp.zeros_like(dwd)

    dwd[...] += dot_tn(hid_s[...], dy_ref[...])


def last_layer(h, dy, wg, wu, wd, t=1024):
    S = jax.ShapeDtypeStruct
    return pl.pallas_call(
        last_kernel,
        grid=(TOK // t,),
        in_specs=[tile(t, D), tile(t, D), full((D, FF)), full((D, FF)), full((FF, D))],
        out_specs=[tile(t, D), tile(t, FF), tile(t, FF), full((FF, D)), pl.BlockSpec((D, t), lambda i: (0, i))],
        out_shape=[S((TOK, D), BF), S((TOK, FF), BF), S((TOK, FF), BF), S((FF, D), F32), S((D, TOK), BF)],
        scratch_shapes=[pltpu.VMEM((t, D), BF), pltpu.VMEM((t, FF), BF)],
        compiler_params=pltpu.CompilerParams(vmem_limit_bytes=66_000_000),
        cost_estimate=pl.CostEstimate(flops=12 * TOK * D * FF, bytes_accessed=80_000_000, transcendentals=TOK * FF),
        name="last_layer",
    )(h, dy, wg, wu, wd)


def hidden_kernel(gate_ref, up_ref, dy_ref, wd, dg_ref, du_ref, dwd, hid_s):
    for lo in range(0, 512, 256):
        r = slice(lo, lo + 256)
        for n in range(7):
            cs = slice(n * 256, (n + 1) * 256)
            back = dot_nt(dy_ref[r], wd[cs]).astype(BF).astype(F32)
            g, u = gate_ref[r, cs], up_ref[r, cs]
            s = sigmoid(g)
            silu = g * s
            hid_s[r, cs] = (silu * u).astype(BF)
            dg_ref[r, cs] = (back * u * (s + silu * (1 - s))).astype(BF)
            du_ref[r, cs] = (back * silu).astype(BF)

    @pl.when(pl.program_id(0) == 0)
    def _():
        dwd[...] = jnp.zeros_like(dwd)

    for lo in range(0, FF, FF // 2):
        r = slice(lo, lo + FF // 2)
        dwd[r] += dot_tn(hid_s[:, r], dy_ref[...])


def hidden_back(gate, up, dy, wd, t=512):
    S = jax.ShapeDtypeStruct
    return pl.pallas_call(
        hidden_kernel,
        grid=(TOK // t,),
        in_specs=[tile(t, FF), tile(t, FF), tile(t, D), full((FF, D))],
        out_specs=[tile(t, FF), tile(t, FF), full((FF, D))],
        out_shape=[S((TOK, FF), BF), S((TOK, FF), BF), S((FF, D), F32)],
        scratch_shapes=[pltpu.VMEM((t, FF), BF)],
        compiler_params=pltpu.CompilerParams(vmem_limit_bytes=66_000_000),
        cost_estimate=pl.CostEstimate(flops=4 * TOK * D * FF, bytes_accessed=100_000_000, transcendentals=TOK * FF),
        name="hidden_back",
    )(gate, up, dy, wd)


def weight_kernel(at, d_ref, o_ref):
    o_ref[...] = dot(at[...], d_ref[...]).astype(BF)


def weight_back(at, d):
    return pl.pallas_call(
        weight_kernel,
        grid=(7,),
        in_specs=[full((D, TOK)), pl.BlockSpec((TOK, 256), lambda i: (0, i))],
        out_specs=pl.BlockSpec((D, 256), lambda i: (0, i)),
        out_shape=jax.ShapeDtypeStruct((D, FF), BF),
        compiler_params=pltpu.CompilerParams(vmem_limit_bytes=40_000_000),
        cost_estimate=pl.CostEstimate(flops=2 * TOK * D * FF, bytes_accessed=22_000_000, transcendentals=0),
        name="weight_back",
    )(at, d)


def input_kernel(dg, du, wg, wu, h_ref, dy_ref, o_ref):
    for lo in range(0, h_ref.shape[0], 256):
        r = slice(lo, lo + 256)
        o_ref[r] = norm_back(dot_nt(dg[r], wg[...]) + dot_nt(du[r], wu[...]), h_ref[r], dy_ref[r])


def input_back(dg, du, wg, wu, h, dy, t=1024):
    return pl.pallas_call(
        input_kernel,
        grid=(TOK // t,),
        in_specs=[tile(t, FF), tile(t, FF), full((D, FF)), full((D, FF)), tile(t, D), tile(t, D)],
        out_specs=tile(t, D),
        out_shape=jax.ShapeDtypeStruct((TOK, D), BF),
        compiler_params=pltpu.CompilerParams(vmem_limit_bytes=60_000_000),
        cost_estimate=pl.CostEstimate(flops=4 * TOK * D * FF, bytes_accessed=60_000_000, transcendentals=0),
        name="input_back",
    )(dg, du, wg, wu, h, dy)


def solution(mesh):
    def summed(term):
        return lax.psum(lax.psum_scatter(term, "s", scatter_dimension=0, tiled=True), "r")

    def step(x, dy, wg, wu, wd):
        x, dy = x[0], dy[0]
        h1, gate, up, at0, w0g, w0u, w0d, w1g, w1u, w1d = forward(x, wg, wu, wd)
        dh, dg1, du1, dwd1, at1 = last_layer(h1, dy, w1g, w1u, w1d)
        by1 = [summed(t) for t in (weight_back(at1, dg1), weight_back(at1, du1), dwd1.astype(BF))]
        dg0, du0, dwd0 = hidden_back(gate, up, dh, w0d)
        by0 = [summed(t) for t in (weight_back(at0, dg0), weight_back(at0, du0), dwd0.astype(BF))]
        by_x = input_back(dg0, du0, w0g, w0u, x, dh)
        return (by_x[None], *(jnp.stack([a, b]) for a, b in zip(by0, by1)))

    states, cut = P(("rep", "r", "s"), None, None), P(None, "s", None)
    return jax.shard_map(
        step,
        mesh=mesh,
        in_specs=(states, states) + (cut,) * 3,
        out_specs=(states,) + (P("rep", "s", None),) * 3,
        check_vma=False,
    )
```

```python
import functools
import jax
import jax.numpy as jnp
from jax import lax
from jax.experimental import pallas as pl
from jax.experimental.pallas import tpu as pltpu
from jax.sharding import PartitionSpec as P

F32, BF = jnp.float32, jnp.bfloat16
TOK, D, FF = 4096, 768, 1792
B = 256
NF = FF // B
TILES = 8
T = TOK // TILES
ANY = pl.BlockSpec(memory_space=pl.ANY)
DMA = pltpu.SemaphoreType.DMA
VMEM_LIMIT = 67_000_000


def dot(a, b):
    return jnp.dot(a, b, preferred_element_type=F32)


def dot_nt(a, b):
    return lax.dot_general(a, b, (((1,), (1,)), ((), ())), preferred_element_type=F32)


def sigmoid(g):
    return 0.5 + 0.5 * jnp.tanh(0.5 * g)


def odd(i):
    return lax.rem(i, 2)


def span(i, n, unit=None):
    return pl.ds(pl.multiple_of(i * n, unit or n), n)


def columns(n):
    return slice(n * B, (n + 1) * B)


def go(copies):
    for copy in copies:
        copy.start()


def done(copies):
    for copy in copies:
        copy.wait()


def local(src, dst, sem):
    return pltpu.make_async_copy(src, dst, sem)


def remote(src, dst, send, recv, to):
    return pltpu.make_async_remote_copy(src_ref=src, dst_ref=dst, send_sem=send, recv_sem=recv, device_id=to, device_id_type=pl.DeviceIdType.MESH)


def meet(peers):
    barrier = pltpu.get_barrier_semaphore()
    for to in peers:
        pl.semaphore_signal(barrier, inc=1, device_id=to, device_id_type=pl.DeviceIdType.MESH)
    return lambda: pl.semaphore_wait(barrier, len(peers))


def place():
    r, s = lax.axis_index("r"), lax.axis_index("s")
    return r // 4, lax.rem(r, 4), s // 2, odd(s)


def in_quad(y, z):
    return {"r": 4 * y + z}


def on_core(x, c):
    return {"s": 2 * x + c}


PARTS = (3, 3, 1, 1, 1, 1)


def forward_kernel(x_hbm, wg_in, wu_in, wd_in,
                   h1_hbm, gate_hbm, up_hbm, at_hbm, hidt_hbm, w0g, w0u, w0d, w1g, w1u, w1d,
                   wg_v, wu_v, wd_v, og, ou, od, a_v, gate_v, hin, up_s, at_s, hid_s, hidt_s, h1_s,
                   sa, sr, sp, sq, so, s_loc, s_hin, s_up, s_at, s_h1, s_gate, s_w0, s_hidt):
    y, z, x, c = place()
    colour = odd(y + z)
    partner, across = on_core(x, 1 - c), on_core(1 - x, c)
    beside = in_quad(1 - y, z), in_quad(y, z + 1 - 2 * odd(z))
    mine, theirs, others = 2 * x + c, 2 * (1 - x) + c, 2 * (1 - x) + 1 - c
    shards = wg_in, wu_in, wd_in
    whole = wg_v, wu_v, wd_v, w1g, w1u, w1d
    rows = tuple(ref.shape[0] // 4 for ref in whole)

    def piece(m, q, half, way, k):
        n = rows[m] // (4 * PARTS[m])
        return span((2 * half + way) * PARTS[m] + k, n, 16), span((4 * q + 2 * half + way) * PARTS[m] + k, n, 16)

    def quarter(m, q):
        return whole[m].at[span(q, rows[m])]

    def sems(table, m, way, k):
        at = 2 * (sum(PARTS[:m]) + k) + way
        return table.at[0, at], table.at[1, at]

    def first(m, way, k):
        src, dst = piece(m, mine, colour, way, k)
        return remote(shards[m % 3].at[m // 3, src], whole[m].at[dst], *sems(sa, m, way, k), across)

    def own(m):
        return remote(shards[m % 3].at[m // 3], quarter(m, mine), so.at[0, m], so.at[1, m], partner)

    def onward(m, q, half, way, k, table, to):
        p = whole[m].at[piece(m, q, half, way, k)[1]]
        return remote(p, p, *sems(table, m, way, k), to)

    def relay(m, way, k):
        return onward(m, theirs, colour, way, k, sr, beside[way])

    def pass_first(m, way, k):
        return onward(m, theirs, colour, way, k, sp, partner)

    def pass_beside(m, way, k):
        return onward(m, theirs, 1 - colour, way, k, sq, partner)

    def every(m):
        return [(m, way, k) for k in range(PARTS[m]) for way in range(2)]

    def at_first(m, way, k):
        onward(m, theirs, colour, way, k, sa, across).wait_recv()
        relay(m, way, k).start()
        pass_first(m, way, k).start()

    def at_beside(m, way, k):
        onward(m, theirs, 1 - colour, way, k, sr, beside[way]).wait_recv()
        pass_beside(m, way, k).start()

    def at_end(m):
        for p in every(m):
            pass_first(*p).wait_recv()
            pass_beside(*p).wait_recv()

    def all_of(f, *matrices):
        for m in matrices:
            for p in every(m):
                f(*p)

    met = meet((partner, across, *beside))
    loads = [local(shards[m].at[n], (quarter(m, mine), (og, ou, od)[m])[n], s_loc.at[n, m]) for n in range(2) for m in range(3)]
    go(loads)

    def load_h(i):
        return local(x_hbm.at[span(i, T)], hin.at[odd(i)], s_hin.at[odd(i)])

    def next_h(i):
        load_h(i).wait()

        @pl.when(i < TILES - 1)
        def _():
            load_h(i + 1).start()

    takes = [local(x_hbm.at[span(i, T)], a_v.at[span(i, T)], s_gate.at[i]) for i in range(TILES)]
    go(takes)
    met()
    for m in range(6):
        own(m).start()
        all_of(lambda *p: first(*p).start(), m)

    @pl.loop(0, TILES)
    def _(i):
        local(x_hbm.at[span(i, T)], a_v.at[span(i, T)], s_gate.at[i]).wait()
        h = a_v[span(i, T)].astype(F32)
        a_v[span(i, T)] = (h * lax.rsqrt(jnp.mean(h * h, -1, keepdims=True) + 1e-6)).astype(BF)

    done(loads)
    saves = [local((og, ou, od)[m], quarter(3 + m, mine), s_loc.at[0, m]) for m in range(3)]
    go(saves)
    own(0).wait_recv()
    order = every(0)

    def in_turn(i, todo):
        for step, work in enumerate(todo):
            @pl.when(i == step)
            def _():
                for f, *p in work:
                    f(*p)

    def halves(i):
        return [span(2 * i + half, T // 2) for half in range(2)]

    @pl.loop(0, TILES)
    def _(i):
        in_turn(i - 1, [[(at_first, *p)] for p in order])
        ks = span(2 * x, B)
        for rs in halves(i):
            for n in range(NF):
                gate_v[rs, columns(n)] = dot(a_v[rs, ks], wg_v[ks, columns(n)])

    all_of(at_beside, 0)
    all_of(at_first, 1)
    at_end(0)
    w0_out = [local(whole[m], (w0g, w0u, w0d)[m], s_w0.at[m]) for m in range(3)]
    w0_out[0].start()

    def store_gate(i):
        return local(gate_v.at[span(i, T)], gate_hbm.at[span(i, T)], s_gate.at[i])

    def store_at(i):
        return local(at_s.at[odd(i)], at_hbm.at[:, span(i, T)], s_at.at[odd(i)])

    def store_hidt(i):
        return local(hidt_s.at[odd(i)], hidt_hbm.at[:, span(i, T)], s_hidt.at[odd(i)])

    def store_up(i):
        return local(up_s.at[odd(i)], up_hbm.at[span(i, T // 2)], s_up.at[odd(i)])

    def store_h1(i):
        return local(h1_s.at[odd(i)], h1_hbm.at[span(i, T)], s_h1.at[odd(i)])

    turns = [[] for _ in range(TILES)]
    for n, p in enumerate(every(1)):
        turns[2 + n].append((at_beside, *p))
    for n, p in enumerate(every(2)):
        turns[5 + 2 * n].append((at_first, *p))

    @pl.loop(0, TILES)
    def _(i):
        in_turn(i, turns)

        @pl.when(i >= 2)
        def _():
            store_at(i - 2).wait()

        ks = pl.ds(pl.multiple_of((1 - x) * B, B), D - B)
        for rs in halves(i):
            for n in range(NF):
                gate_v[rs, columns(n)] += dot(a_v[rs, ks], wg_v[ks, columns(n)])
        at_s[odd(i)] = a_v[span(i, T)].T
        store_gate(i).start()
        store_at(i).start()

    at_end(1)
    own(1).wait_recv()
    w0_out[1].start()
    load_h(0).start()

    def up_tile(i):
        for half, rs in enumerate(halves(i)):
            j = 2 * i + half

            @pl.when(j >= 2)
            def _():
                store_up(j - 2).wait()

            a = a_v[rs]
            for n in range(NF):
                cs = columns(n)
                g = gate_v[rs, cs]
                u = dot(a, wu_v[:, cs])
                up_s[half, :, cs] = u
                hid_s[lax.rem(i, LAG_DOWN + 1), half * (T // 2):(half + 1) * (T // 2), cs] = (g * sigmoid(g) * u).astype(BF)
            store_up(j).start()

    def down_tile(i):
        k = odd(i)
        for half in range(2):
            rs = slice(half * (T // 2), (half + 1) * (T // 2))
            h1_s[k, rs] = hin[k, rs] + dot(hid_s[lax.rem(i, LAG_DOWN + 1), rs], wd_v[...]).astype(BF)
        hidt_s[k] = hid_s[lax.rem(i, LAG_DOWN + 1)].T
        store_h1(i).start()
        store_hidt(i).start()

    turns = [[] for _ in range(TILES)]
    for n, p in enumerate(every(2)):
        turns[LAG_DOWN - 1].append((at_beside, *p))
    for n, m in enumerate((3, 4, 5)):
        turns[1 + 2 * n] += [(at_first, *p) for p in every(m)]
        turns[3 + 2 * n] += [(at_beside, *p) for p in every(m)]

    @pl.loop(0, LAG_DOWN)
    def _(i):
        in_turn(i, turns[:LAG_DOWN])
        up_tile(i)

    at_end(2)
    own(2).wait_recv()
    w0_out[2].start()

    @pl.loop(LAG_DOWN, TILES + LAG_DOWN)
    def _(i):
        j = i - LAG_DOWN
        in_turn(j, turns[LAG_DOWN:])
        next_h(j)

        @pl.when(j >= 2)
        def _():
            store_h1(j - 2).wait()
            store_hidt(j - 2).wait()

        @pl.when(i < TILES)
        def _():
            up_tile(i)

        down_tile(j)

    for m in (3, 4, 5):
        at_end(m)
        own(m).wait_recv()
    for i in (TILES - 2, TILES - 1):
        done((store_h1(i), store_hidt(i), store_at(i), store_up(TILES + i)))
    for i in range(TILES):
        store_gate(i).wait()
    done(w0_out + saves)
    for m in range(6):
        own(m).wait_send()
        for f in (first, relay, pass_first, pass_beside):
            all_of(lambda *p: f(*p).wait_send(), m)


LAG_DOWN = 2


def forward(x, wg, wu, wd):
    S = jax.ShapeDtypeStruct
    V = pltpu.VMEM
    wide, deep = (D, FF), (FF, D)
    weights = [S(wide, BF), S(wide, BF), S(deep, BF)]
    pieces = (2, 2 * sum(PARTS))
    return pl.pallas_call(
        forward_kernel,
        out_shape=[S((TOK, D), BF), S((TOK, FF), F32), S((TOK, FF), F32), S((D, TOK), BF), S((FF, TOK), BF)] + weights + weights,
        in_specs=[ANY] * 4,
        out_specs=[ANY] * 11,
        scratch_shapes=[
            V(wide, BF), V(wide, BF), V(deep, BF), V(wg.shape[1:], BF), V(wu.shape[1:], BF), V(wd.shape[1:], BF),
            V((TOK, D), BF), V((TOK, FF), F32), V((2, T, D), BF), V((2, T // 2, FF), F32), V((2, D, T), BF),
            V((LAG_DOWN + 1, T, FF), BF), V((2, FF, T), BF), V((2, T, D), BF),
            *[DMA(pieces)] * 4, DMA((2, 6)), DMA((2, 3)), *[DMA((2,))] * 4, DMA((TILES,)), DMA((3,)), DMA((2,)),
        ],
        compiler_params=pltpu.CompilerParams(collective_id=0, has_side_effects=True, vmem_limit_bytes=VMEM_LIMIT),
        cost_estimate=pl.CostEstimate(flops=6 * TOK * D * FF, bytes_accessed=130_000_000, transcendentals=TOK * FF),
        name="forward",
    )(x, wg, wu, wd)


def dot_tn(a, b):
    return lax.dot_general(a, b, (((0,), (0,)), ((), ())), preferred_element_type=F32)

MESH = pl.DeviceIdType.MESH
def place4():
    r, s = lax.axis_index("r"), lax.axis_index("s")
    return r, r // 4, lax.rem(r, 4), s, s // 2, lax.rem(s, 2)


def full(shape):
    return pl.BlockSpec(shape, lambda i: (0,) * len(shape), pipeline_mode=pl.Buffered(1))


def tile(t, n):
    return pl.BlockSpec((t, n), lambda i: (i, 0))


def norm_back(da, h, dy):
    h, da = h.astype(F32), da.astype(BF).astype(F32)
    scale = lax.rsqrt(jnp.mean(h * h, -1, keepdims=True) + 1e-6)
    along = jnp.sum(da * h, -1, keepdims=True) * (scale * scale * scale * (1.0 / D))
    return dy + (da * scale - h * along).astype(BF)


def last_kernel(h_ref, dy_ref, wg, wu, wd, dh_ref, dg_ref, du_ref, hidt_ref, at_ref, a_s, hid_s):
    n_rows = h_ref.shape[0]
    for lo in range(0, n_rows, 512):
        r = slice(lo, lo + 512)
        h = h_ref[r].astype(F32)
        a_s[r] = (h * lax.rsqrt(jnp.mean(h * h, -1, keepdims=True) + 1e-6)).astype(BF)
    for lo in range(0, n_rows, 512):
        r = slice(lo, lo + 512)
        for n in range(NF):
            cs = columns(n)
            g, u = dot(a_s[r], wg[:, cs]), dot(a_s[r], wu[:, cs])
            back = dot_nt(dy_ref[r], wd[cs]).astype(BF).astype(F32)
            s = sigmoid(g)
            silu = g * s
            hid_s[r, cs] = (silu * u).astype(BF)
            dg_ref[r, cs] = (back * u * (s + silu * (1 - s))).astype(BF)
            du_ref[r, cs] = (back * silu).astype(BF)
    for lo in range(0, n_rows, 256):
        r = slice(lo, lo + 256)
        dh_ref[r] = norm_back(dot_nt(dg_ref[r], wg[...]) + dot_nt(du_ref[r], wu[...]), h_ref[r], dy_ref[r])
    at_ref[...] = a_s[...].T
    hidt_ref[...] = hid_s[...].T


def last_layer(h, dy, wg, wu, wd, t=1024):
    S = jax.ShapeDtypeStruct
    return pl.pallas_call(
        last_kernel,
        grid=(TOK // t,),
        in_specs=[tile(t, D), tile(t, D), full((D, FF)), full((D, FF)), full((FF, D))],
        out_specs=[tile(t, D), tile(t, FF), tile(t, FF), pl.BlockSpec((FF, t), lambda i: (0, i)), pl.BlockSpec((D, t), lambda i: (0, i))],
        out_shape=[S((TOK, D), BF), S((TOK, FF), BF), S((TOK, FF), BF), S((FF, TOK), BF), S((D, TOK), BF)],
        scratch_shapes=[pltpu.VMEM((t, D), BF), pltpu.VMEM((t, FF), BF)],
        compiler_params=pltpu.CompilerParams(vmem_limit_bytes=66_000_000),
        cost_estimate=pl.CostEstimate(flops=12 * TOK * D * FF, bytes_accessed=80_000_000, transcendentals=TOK * FF),
        name="last_layer",
    )(h, dy, wg, wu, wd)


OUT = (jax.ShapeDtypeStruct((2, 192, FF), BF),) * 2 + (jax.ShapeDtypeStruct((2, 448, D), BF),)
UNITS = 42
LAG = (0, 2, 5, 7, 10, 13, 15, 16)
HT = TOK // 16
SLOTS, QUARTER, HALF = 8, 64, D // 2
ND = 14


def gradient_kernel(dy_hbm, dh_hbm, x_hbm, at1, hidt1, dg1, du1, at0, hidt0, gate0, up0, w0g, w0u, w0d,
                    gg, gu, gd, dg0, du0, dx_hbm,
                    at_v, dy_v, hbuf, cbuf, gate_v, up_v, dht_v, dgo, duo, wd_v, wg_v, wu_v, xt_v, dxo, term,
                    snd0, rcv0, keep1, snd1, rcv1, keep2, snd2, rcv2, keep3, snd3, rcv3, fin,
                    s_at, s_dy, s_h, s_c, s_g, s_u, s_dh, s_dgo, s_duo, s_w, s_x, s_dx,
                    s0, s1, s2, s3, s4, s5, s_out):
    r, y, z, s, x, c = place4()
    partner = {"s": 2 * x + (1 - c)}
    across = {"s": 2 * (1 - x) + c}
    ypeer = {"r": lax.rem(r + 4, 8)}
    zs = [lax.rem(z + d, 4) for d in (1, 2, 3)]
    zpeers = [{"r": 4 * y + zz} for zz in zs]

    def remote(src, dst, sems, to):
        return pltpu.make_async_remote_copy(src_ref=src, dst_ref=dst, send_sem=sems[0], recv_sem=sems[1], device_id=to, device_id_type=MESH)

    def pair(sems, *at):
        return sems.at[(0, *at)], sems.at[(1, *at)]

    def to_partner(v):
        k = lax.rem(v, 4)
        return remote(snd0.at[k], rcv0.at[k], pair(s0, k), partner)

    def to_across(v):
        k = lax.rem(v, SLOTS)
        return remote(snd1.at[k], rcv1.at[k], pair(s1, k), across)

    def to_y(v):
        k = lax.rem(v, SLOTS)
        return remote(snd2.at[k], rcv2.at[k], pair(s2, k), ypeer)

    def to_z(v):
        k = lax.rem(v, SLOTS)
        return [remote(snd3.at[k, span(zz, 16)], rcv3.at[k, d], pair(s3, k, d), to)
                for d, (zz, to) in enumerate(zip(zs, zpeers))]

    def back_z(v):
        k = lax.rem(v, 16)
        p = fin.at[k, y, span(z, 16)]
        return [remote(p, p, pair(s4, k, d), to) for d, to in enumerate(zpeers)]

    def back_y(v):
        k = lax.rem(v, 16)
        return remote(fin.at[k, y], fin.at[k, y], pair(s5, k), ypeer)

    def half(i):
        return span(i, HALF, 128)

    def stage1(v):
        to_partner(v).wait()
        k, k1 = lax.rem(v, 4), lax.rem(v, SLOTS)
        keep1[k1] = term[k, 2 * x + c] + rcv0[k, x].astype(F32)
        snd1[k1] = (term[k, 2 * (1 - x) + c] + rcv0[k, 1 - x].astype(F32)).astype(BF)
        to_across(v).start()

    def stage2(v):
        to_across(v).wait()
        k = lax.rem(v, SLOTS)
        keep2[k] = keep1[k, :, half(y)] + rcv1[k, :, half(y)].astype(F32)
        snd2[k] = (keep1[k, :, half(1 - y)] + rcv1[k, :, half(1 - y)].astype(F32)).astype(BF)
        to_y(v).start()

    def stage3(v):
        to_y(v).wait()
        k = lax.rem(v, SLOTS)
        mine = span(z, 16)
        keep3[k] = keep2[k, mine] + rcv2[k, mine].astype(F32)
        snd3[k] = (keep2[k] + rcv2[k].astype(F32)).astype(BF)
        for copy in to_z(v):
            copy.start()

    def stage4(v):
        for copy in to_z(v):
            copy.wait()
        k = lax.rem(v, SLOTS)
        total = keep3[k]
        for d in range(3):
            total = total + rcv3[k, d].astype(F32)
        fin[lax.rem(v, 16), y, span(z, 16)] = total.astype(BF)
        for copy in back_z(v):
            copy.start()

    def stage5(v):
        for copy in back_z(v):
            copy.wait()
        back_y(v).start()

    def outward(v):
        k, n, layer = lax.rem(v, 16), lax.rem(v, 21) // 3, 1 - v // 21
        kind = lax.rem(v, 3)
        to_down = [pltpu.make_async_copy(fin.at[k, h], gd.at[layer, span(n, QUARTER), h * 384:(h + 1) * 384], s_out.at[k, h])
                   for h in range(2)]
        plans = [(kind == 0, to_down)]
        for m, ref in ((1, gg), (2, gu)):
            todo = []
            for i, (h, lo, width, row, at) in enumerate(((0, 0, 256, 0, 0), (0, 256, 128, 64, 0), (1, 0, 128, 64, 128), (1, 128, 256, 128, 0))):
                dst = ref.at[layer, row:row + 64, pl.ds(pl.multiple_of(256 * n + at, 128), width)]
                todo.append(pltpu.make_async_copy(fin.at[k, h, :, lo:lo + width], dst, s_out.at[k, i]))
            plans.append((kind == m, todo))
        return plans

    def stage6(v):
        back_y(v).wait()
        for chosen, copies in outward(v):
            @pl.when(chosen)
            def _():
                for copy in copies:
                    copy.start()

    def stage7(v):
        for chosen, copies in outward(v):
            @pl.when(chosen)
            def _():
                for copy in copies:
                    copy.wait()

    stages = (stage1, stage2, stage3, stage4, stage5, stage6, stage7)

    def exchange(t):
        for n in range(7, 0, -1):
            v = t - LAG[n]

            @pl.when((v >= 0) & (v < UNITS))
            def _():
                stages[n - 1](v)

    def send_off(v):
        k = lax.rem(v, 4)
        for j in range(2):
            snd0[k, j] = term[k, 2 * j + 1 - c].astype(BF)
        to_partner(v).start()

    def rows(ref, i):
        return ref.at[span(i, HT)]

    def loads_back(i):
        k = odd(i)
        return [pltpu.make_async_copy(rows(gate0, i), gate_v.at[k], s_g.at[k]), pltpu.make_async_copy(rows(up0, i), up_v.at[k], s_u.at[k]),
                pltpu.make_async_copy(rows(dh_hbm, i), dht_v.at[k], s_dh.at[k])]

    def stores_back(i):
        k = odd(i)
        return [pltpu.make_async_copy(dgo.at[k], rows(dg0, i), s_dgo.at[k]), pltpu.make_async_copy(duo.at[k], rows(du0, i), s_duo.at[k])]

    def loads_input(i):
        k = odd(i)
        return [pltpu.make_async_copy(rows(dg0, i), dgo.at[k], s_g.at[k]), pltpu.make_async_copy(rows(du0, i), duo.at[k], s_u.at[k]),
                pltpu.make_async_copy(rows(dh_hbm, i), dht_v.at[k], s_dh.at[k]), pltpu.make_async_copy(rows(x_hbm, i), xt_v.at[k], s_x.at[k])]

    def store_input(i):
        k = odd(i)
        return pltpu.make_async_copy(dxo.at[k], rows(dx_hbm, i), s_dx.at[k])

    def load_rows(src, n):
        return [pltpu.make_async_copy(src.at[span(NF * q + n, QUARTER)], hbuf.at[QUARTER * q:QUARTER * (q + 1)], s_h.at[q])
                for q in range(4)]

    def load_columns(src, n, k):
        return pltpu.make_async_copy(src.at[:, span(n, B)], cbuf.at[k], s_c.at[k])

    def go(copies):
        for copy in copies:
            copy.start()

    def done(copies):
        for copy in copies:
            copy.wait()

    def ready_back(i):
        @pl.when(i + 1 < 16)
        def _():
            go(loads_back(i + 1))

        done(loads_back(i))

        @pl.when(i >= 2)
        def _():
            done(stores_back(i - 2))

    def back(i):
        k = odd(i)
        for n in range(7):
            cs = columns(n)
            by = dot_nt(dht_v[k], wd_v[cs]).astype(BF).astype(F32)
            g, u = gate_v[k, :, cs], up_v[k, :, cs]
            sg = sigmoid(g)
            silu = g * sg
            dgo[k, :, cs] = (by * u * (sg + silu * (1 - sg))).astype(BF)
            duo[k, :, cs] = (by * silu).astype(BF)

    def down_unit(v):
        slot = lax.rem(v, 4)
        for p in range(2):
            o = dot(hbuf[128 * p:128 * (p + 1)], dy_v[...])
            for q in range(2):
                term[slot, 2 * p + q] = o[64 * q:64 * (q + 1)]

    def column_unit(v, k):
        slot = lax.rem(v, 4)
        for p in range(2):
            o = dot(at_v[384 * p:384 * (p + 1)], cbuf[k])
            for q in range(2):
                for b in range(3):
                    lo = 192 * q + 64 * b
                    term[slot, 2 * p + q, :, 256 * b:256 * (b + 1)] = o[lo:lo + 64]

    barrier = pltpu.get_barrier_semaphore()
    for to in (partner, across, ypeer, *zpeers):
        pl.semaphore_signal(barrier, inc=1, device_id=to, device_id_type=MESH)
    go(loads_back(0))
    load_wd = pltpu.make_async_copy(w0d, wd_v, s_w.at[0])
    load_wg = pltpu.make_async_copy(w0g, wg_v, s_w.at[1])
    load_wu = pltpu.make_async_copy(w0u, wu_v, s_w.at[2])
    load_wd.start()
    load_dy = pltpu.make_async_copy(dy_hbm, dy_v, s_dy)
    load_dh = pltpu.make_async_copy(dh_hbm, dy_v, s_dy)
    load_at1 = pltpu.make_async_copy(at1, at_v, s_at)
    load_at0 = pltpu.make_async_copy(at0, at_v, s_at)
    ready_back(0)
    load_dy.start()
    go(load_rows(hidt1, 0))
    load_wd.wait()
    back(0)
    go(stores_back(0))
    ready_back(1)
    back(1)
    go(stores_back(1))
    load_at1.start()
    for k, src in enumerate((dg1, du1)):
        load_columns(src, 0, k).start()
    pl.semaphore_wait(barrier, 6)
    load_dy.wait()

    def rest(n, layer, sources, k):
        v = 21 * (1 - layer) + 3 * n + 1 + k
        exchange(v)
        load_columns(sources[k], n, k).wait()
        if layer:
            i = 2 * (n + 1) + k
            ready_back(i)
            column_unit(v, k)
            back(i)
            go(stores_back(i))
        else:
            column_unit(v, k)
        send_off(v)

        @pl.when(n < 6)
        def _():
            load_columns(sources[k], n + 1, k).start()

    @pl.loop(0, 7)
    def _(n):
        exchange(3 * n)
        done(load_rows(hidt1, n))
        down_unit(3 * n)
        send_off(3 * n)

        @pl.when(n < 6)
        def _():
            go(load_rows(hidt1, n + 1))

        @pl.when(n == 0)
        def _():
            load_at1.wait()

        @pl.when(n == 6)
        def _():
            load_dh.start()
            go(load_rows(hidt0, 0))

        for k in range(2):
            rest(n, 1, (dg1, du1), k)

    done(stores_back(14))
    done(stores_back(15))
    load_at0.start()
    for k, src in enumerate((dg0, du0)):
        load_columns(src, 0, k).start()
    load_wg.start()
    load_wu.start()
    load_dh.wait()

    @pl.loop(0, 7)
    def _(n):
        exchange(21 + 3 * n)
        done(load_rows(hidt0, n))
        down_unit(21 + 3 * n)
        send_off(21 + 3 * n)

        @pl.when(n < 6)
        def _():
            go(load_rows(hidt0, n + 1))

        @pl.when(n == 0)
        def _():
            load_at0.wait()

        @pl.when(n == 6)
        def _():
            go(loads_input(0))

        for k in range(2):
            rest(n, 0, (dg0, du0), k)

    load_wg.wait()
    load_wu.wait()

    @pl.loop(0, ND)
    def _(i):
        k = odd(i)

        @pl.when(i + 1 < ND)
        def _():
            go(loads_input(i + 1))

        exchange(42 + i)
        done(loads_input(i))

        @pl.when(i >= 2)
        def _():
            store_input(i - 2).wait()

        dxo[k] = norm_back(dot_nt(dgo[k], wg_v[...]) + dot_nt(duo[k], wu_v[...]), xt_v[k], dht_v[k])
        store_input(i).start()

    for i in (ND - 2, ND - 1):
        store_input(i).wait()

    @pl.loop(UNITS + ND, UNITS + LAG[7])
    def _(t):
        exchange(t)


def gradients(dy, dh, x, at1, hidt1, dg1, du1, at0, hidt0, gate0, up0, w0g, w0u, w0d):
    S = jax.ShapeDtypeStruct
    V = pltpu.VMEM

    def two(n, dtype=BF):
        return V((2, HT, n), dtype)

    def slots(n, dtype=BF, rows=QUARTER, parts=None):
        if parts:
            return V((4 if rows == QUARTER else SLOTS, parts, rows, n), dtype)
        return V((SLOTS, rows, n), dtype)

    return pl.pallas_call(
        gradient_kernel,
        out_shape=OUT + (S((TOK, FF), BF), S((TOK, FF), BF), S((TOK, D), BF)),
        in_specs=[ANY] * 14,
        out_specs=(ANY,) * 6,
        scratch_shapes=[
            V((D, TOK), BF), V((TOK, D), BF), V((B, TOK), BF), V((2, TOK, B), BF), two(FF, F32), two(FF, F32),
            two(D), two(FF), two(FF), V((FF, D), BF), V((D, FF), BF), V((D, FF), BF),
            two(D), two(D), slots(D, F32, QUARTER, 4),
            slots(D, BF, QUARTER, 2), slots(D, BF, QUARTER, 2), slots(D, F32), slots(D), slots(D),
            slots(HALF, F32), slots(HALF), slots(HALF), slots(HALF, F32, QUARTER // 4), slots(HALF), slots(HALF, BF, QUARTER // 4, 3),
            V((2 * SLOTS, 2, QUARTER, HALF), BF),
            DMA, DMA, DMA((4,)), *[DMA((2,))] * 6, DMA((3,)), *[DMA((2,))] * 2,
            *[DMA((2, SLOTS))] * 3, DMA((2, SLOTS, 3)), DMA((2, 2 * SLOTS, 3)), DMA((2, 2 * SLOTS)), DMA((2 * SLOTS, 4)),
        ],
        compiler_params=pltpu.CompilerParams(collective_id=1, has_side_effects=True, vmem_limit_bytes=67_000_000),
        cost_estimate=pl.CostEstimate(flops=18 * TOK * D * FF, bytes_accessed=250_000_000, transcendentals=TOK * FF),
        name="gradients",
    )(dy, dh, x, at1, hidt1, dg1, du1, at0, hidt0, gate0, up0, w0g, w0u, w0d)


def finish_kernel(dx_in, gg, gu, gd, dg, du, wg, wu, h_ref, dh_ref, dx, ggo, guo, gdo, dx_v, gg_v, gu_v, gd_v, dxo, s_in, s_o, s_dx):
    i = pl.program_id(0)
    last = pl.num_programs(0) - 1
    head = pl.ds(0, ND * HT)
    takes = [pltpu.make_async_copy(a, b, s_in.at[n]) for n, (a, b) in enumerate(((dx_in.at[head], dx_v), (gg, gg_v), (gu, gu_v), (gd, gd_v)))]
    puts = [pltpu.make_async_copy(a, b, s_o.at[n]) for n, (a, b) in enumerate(((dx_v, dx.at[head]), (gg_v, ggo), (gu_v, guo), (gd_v, gdo)))]

    def store(j):
        return pltpu.make_async_copy(dxo.at[odd(j)], dx.at[span(ND + j, HT)], s_dx.at[odd(j)])

    @pl.when(i == 0)
    def _():
        for copy in takes:
            copy.start()

    @pl.when(i == last)
    def _():
        for copy in takes:
            copy.wait()
        for copy in puts:
            copy.start()

    @pl.when(i >= 2)
    def _():
        store(i - 2).wait()

    dxo[odd(i)] = norm_back(dot_nt(dg[...], wg[...]) + dot_nt(du[...], wu[...]), h_ref[...], dh_ref[...])
    store(i).start()

    @pl.when(i == last)
    def _():
        store(i - 1).wait()
        store(i).wait()
        for copy in puts:
            copy.wait()


def finish(dx_in, gg, gu, gd, dg, du, wg, wu, h, dh):
    S = jax.ShapeDtypeStruct
    V = pltpu.VMEM
    def at(n):
        return pl.BlockSpec((HT, n), lambda i: (i + ND, 0))
    return pl.pallas_call(
        finish_kernel,
        grid=(16 - ND,),
        in_specs=[ANY] * 4 + [at(FF), at(FF), full((D, FF)), full((D, FF)), at(D), at(D)],
        out_specs=(ANY,) * 4,
        out_shape=(S((TOK, D), BF),) + OUT,
        scratch_shapes=[V((ND * HT, D), BF), *[V(o.shape, BF) for o in OUT], V((2, HT, D), BF), DMA((4,)), DMA((4,)), DMA((2,))],
        compiler_params=pltpu.CompilerParams(vmem_limit_bytes=66_000_000),
        cost_estimate=pl.CostEstimate(flops=TOK * D * FF, bytes_accessed=40_000_000, transcendentals=0),
        name="finish",
    )(dx_in, gg, gu, gd, dg, du, wg, wu, h, dh)


def solution(mesh):
    def step(x, dy, wg, wu, wd):
        x, dy = x[0], dy[0]
        h1, gate, up, at0, hidt0, w0g, w0u, w0d, w1g, w1u, w1d = forward(x, wg, wu, wd)
        dh, dg1, du1, hidt1, at1 = last_layer(h1, dy, w1g, w1u, w1d)
        gg, gu, gd, dg0, du0, dx = gradients(dy, dh, x, at1, hidt1, dg1, du1, at0, hidt0, gate, up, w0g, w0u, w0d)
        dx, gg, gu, gd = finish(dx, gg, gu, gd, dg0, du0, w0g, w0u, x, dh)
        return dx[None], gg, gu, gd

    states, cut = P(("rep", "r", "s"), None, None), P(None, "s", None)
    return jax.shard_map(
        step,
        mesh=mesh,
        in_specs=(states, states) + (cut,) * 3,
        out_specs=(states,) + (P("rep", "s", None),) * 3,
        check_vma=False,
    )
```
